256 devices in a mesh: gx: 4 (over y), gy: 8 (over x, core), gz: 8 (over z).
Axes of the slice: x: 4, y: 4, z: 8, core: 2. Of those that a mesh axis runs over, the one named last changes fastest.
Arguments:
- positions: float32 [3, 4, 8, 8, 128], P(None, 'gx', 'gy', 'gz'), may hold values from 0 to 22
- elements: int32 [4, 8, 8, 128], P('gx', 'gy', 'gz'), may hold values from 0 to 3
- prior_charges: float32 [4, 8, 8, 128], P('gx', 'gy', 'gz'), may hold values from -1.8 to 1.8
- neighbours: int32 [4, 8, 8, 128, 128], P('gx', 'gy', 'gz'), may hold values from 0 to 959, all different within a row; in each aligned block of 128 rows (0 to 127, 128 to 255, ..., all dimensions but the last counted through in order) at most 19 rows name the same one
- counts: int32 [4, 8, 8, 128], P('gx', 'gy', 'gz'), may hold values from 64 to 128
- boundary: int32 [4, 8, 8, 32], P('gx', 'gy', 'gz'), may hold values from 0 to 127, as said below
- wave_numbers: int32 [3, 2048], replicated, may hold values from -6 to 6, as said below
- hardness: float32 [4], replicated, may hold values from 3 to 9
- chi_first: bfloat16 [4, 32, 128], replicated, may hold values from -0.5 to 0.5
- chi_bias: float32 [4, 32], replicated, may hold values from -3 to 3
- chi_mid: bfloat16 [32, 4, 32], replicated, may hold values from -1 to 1
- chi_out: float32 [4, 32], replicated, may hold values from -1 to 1
- chi_offset: float32 [4], replicated, may hold values from -3 to 3
- short_first: bfloat16 [4, 32, 256], replicated, may hold values from -0.375 to 0.375
- short_charge: float32 [4, 32], replicated, may hold values from -4 to 4
- short_bias: float32 [4, 32], replicated, may hold values from -3 to 3
- short_mid: bfloat16 [32, 4, 32], replicated, may hold values from -1 to 1
- short_out: float32 [4, 32], replicated, may hold values from -1 to 1
- short_offset: float32 [4], replicated, may hold values from -3 to 3
Outputs:
- charges: float32 [4, 8, 8, 128], P('gx', 'gy', 'gz')
- energies: float32 [4, 8, 8, 128], P('gx', 'gy', 'gz')
The draws below stay inside these ranges and needn't reach their ends.
Inputs may be any that keep to these rules, and one draw needn't show every extreme that they name: `neighbours`: each row names 128 different indices; within one domain no index is named by more than 19 rows, a bound that some block reaches. `boundary`: the 32 indices of a domain are different. `wave_numbers`: every entry is nonzero.
All inputs are finite; a program needn't handle non-finite values.
Results may differ from the reference program's by a relative error of at most 0.0014.
Values sent between devices are 32-bit elements; how exact they have to be, the bound alone decides.
A program may use at most 64 MiB of HBM per device.

```python
import math
import jax
import jax.numpy as jnp
import numpy as np
from jax import lax

ATOMS_DEV = 128
GHOST = 32
NBR = 128
NB_MOST = 19
ELEM = 4
NBASIS = 32
FEAT = 128
HID = 32
KVEC = 2048
ITERS = 3
NGX = 4
NGY = 8
NGZ = 8


def draw_boundary(key, part):
    base = jax.random.fold_in(key, 17)
    keys = jax.random.split(base, NGX * NGY * NGZ)
    orders = jax.vmap(lambda single: jax.random.permutation(single, ATOMS_DEV))(keys)
    return orders[:, :GHOST].reshape(NGX, NGY, NGZ, GHOST).astype(jnp.int32)


def draw_wave_numbers(key, part):
    base = jax.random.fold_in(key, 29)
    size_key, sign_key = jax.random.split(base)
    magnitude = jax.random.randint(size_key, (3, KVEC), 1, 7)
    signs = jax.random.randint(sign_key, (3, KVEC), 0, 2) * 2 - 1
    return (magnitude * signs).astype(jnp.int32)


def with_ends(entries, rng, low, high):
    longest = entries.shape.index(max(entries.shape))
    spots = []
    for shift in (0, 1):
        where = [jax.random.randint(jax.random.fold_in(rng, axis), (), 0, length) for axis, length in enumerate(entries.shape)]
        where[longest] = (where[longest] + shift) % entries.shape[longest]
        spots.append(tuple(where))
    return entries.at[spots[0]].set(low).at[spots[1]].set(high)


def level_of(rng, extent, pieces, smallest, largest):
    loudness, own = 1.0, jax.random.fold_in(rng, 6)
    for axis_at, blocks in pieces:
        heights = jnp.exp(jax.random.uniform(jax.random.fold_in(own, axis_at), (blocks,), jnp.float32, smallest / len(pieces), largest / len(pieces)))
        loudness = loudness * jnp.repeat(heights, extent[axis_at] // blocks).reshape([-1 if axis == axis_at else 1 for axis in range(len(extent))])
    return loudness


def routed_block(stream_key, own, number, rows, number_of, top, reach, slope):
    ranking = jax.random.permutation(stream_key, number_of)
    crowded, usual = portions_of(number_of, rows * top, reach, slope, True), portions_of(number_of, rows * top, reach, slope, False)
    places = jnp.arange(number_of)

    def named(lengths, rotation):
        used = int((lengths > 0).sum())
        fixed = max(1, used // 4)
        moved = fixed + (places - fixed + rotation * (used - fixed)) % max(1, number_of - fixed)
        return jnp.zeros((number_of,), jnp.int32).at[ranking[jnp.where(places < fixed, places, moved)]].set(jnp.asarray(lengths, jnp.int32))

    lengths = jnp.where(number % 4 == 0, named(crowded, number // 4), named(usual, number - number // 4 - 1))
    mixed = jax.random.permutation(jax.random.fold_in(own, 3), number_of)
    donor, sink = mixed[0:number_of // 2 * 2:2], mixed[1:number_of // 2 * 2:2]
    slack = jnp.minimum(lengths[donor] - 1, reach - lengths[sink]) // 2
    slack = jnp.where((donor == ranking[0]) | (sink == ranking[0]) | (lengths[sink] == 0), 0, jnp.maximum(slack, 0))
    moved = jax.random.randint(jax.random.fold_in(own, 4), (number_of // 2,), 0, 1 << 20) % (slack + 1)
    lengths = lengths.at[donor].add(-moved).at[sink].add(moved)
    members = jnp.searchsorted(jnp.cumsum(lengths), jnp.arange(rows * top), side="right").astype(jnp.int32)
    table = members.reshape(top, rows).T
    table = table[jax.random.permutation(jax.random.fold_in(own, 1), rows)]
    rotation = jax.random.randint(jax.random.fold_in(own, 2), (rows, 1), 0, top)
    return jnp.take_along_axis(table, (jnp.arange(top)[None, :] + rotation) % top, axis=1)


def portions_of(number_of, total, limit, skew, full):
    weights = [(1 << 20) // math.isqrt(rank ** skew) + 1 for rank in range(1, number_of + 1)]
    largest = limit if full else min(limit, max(-(-total // number_of), total * weights[0] // sum(weights)))
    least = 1 if total - largest >= number_of - 1 else 0
    given, surplus = [largest] + [least] * (number_of - 1), total - largest - least * (number_of - 1)
    while surplus > 0:
        movable = [i for i in range(1, number_of) if given[i] < largest] or [i for i in range(1, number_of) if given[i] < limit]
        pool, left = sum([weights[i] for i in movable]), surplus
        for i in movable:
            more = min(limit - given[i], max(1, left * weights[i] // pool), surplus)
            given[i] = given[i] + more
            surplus = surplus - more
    return np.array(given)


def centred(own_key, extent, deviation, reach, pieces=(), kind=jnp.bfloat16):
    values = deviation * jax.random.normal(own_key, extent, jnp.float32)
    if pieces:
        values = values * level_of(own_key, extent, pieces, -0.22, 0.18)
    return jnp.clip(values, -reach, reach).astype(kind)


def setup_inputs(seed: int = 0) -> dict:
    splits = jax.random.split(jax.random.key(seed), 20)
    positions = jnp.clip(22.0 * jax.random.uniform(splits[0], (3, NGX, NGY, NGZ, ATOMS_DEV), jnp.float32) ** level_of(splits[0], (3, NGX, NGY, NGZ, ATOMS_DEV), ((1, 4), (2, 8), (3, 8)), -0.2, 0.2), 0.0, 22.0)
    elements = with_ends(jax.random.randint(splits[1], (NGX, NGY, NGZ, ATOMS_DEV), 0, ELEM), jax.random.fold_in(splits[1], 1), 0, ELEM - 1).astype(jnp.int32)
    prior_charges = centred(splits[2], (NGX, NGY, NGZ, ATOMS_DEV), 0.3, 1.8, ((0, 4), (1, 8), (2, 8)), jnp.float32)
    neighbours_keys = jax.random.split(jax.random.fold_in(splits[3], 1), NGX * NGY * NGZ * ATOMS_DEV // ATOMS_DEV)
    neighbours_turns = jax.random.permutation(jax.random.fold_in(splits[3], 3), NGX * NGY * NGZ * ATOMS_DEV // ATOMS_DEV)
    neighbours = jax.vmap(lambda own, number: routed_block(jax.random.fold_in(splits[3], 2), own, number, ATOMS_DEV, ATOMS_DEV + 26 * GHOST, NBR, NB_MOST, 0))(neighbours_keys, neighbours_turns).reshape((NGX, NGY, NGZ, ATOMS_DEV, NBR))
    counts = with_ends(jax.random.randint(splits[4], (NGX, NGY, NGZ, ATOMS_DEV), NBR // 2, NBR + 1), jax.random.fold_in(splits[4], 1), NBR // 2, NBR).astype(jnp.int32)
    boundary = draw_boundary(jax.random.fold_in(splits[19], 71), 0)
    wave_numbers = draw_wave_numbers(jax.random.fold_in(splits[19], 71), 0)
    hardness = jnp.clip(jnp.exp(jax.random.uniform(splits[7], (ELEM,), jnp.float32, math.log(3.0), math.log(9.0))), 3.0, 9.0)
    chi_first = centred(splits[8], (ELEM, HID, FEAT), FEAT ** -0.5, 0.5)
    chi_bias = centred(splits[9], (ELEM, HID), 0.5, 3.0, (), jnp.float32)
    chi_mid = centred(splits[10], (HID, ELEM, HID), HID ** -0.5, 1.0)
    chi_out = centred(splits[11], (ELEM, HID), HID ** -0.5, 1.0, (), jnp.float32)
    chi_offset = centred(splits[12], (ELEM,), 1.0, 3.0, (), jnp.float32)
    short_first = centred(splits[13], (ELEM, HID, 2 * FEAT), (2 * FEAT) ** -0.5, 0.375)
    short_charge = centred(splits[14], (ELEM, HID), 1.0, 4.0, (), jnp.float32)
    short_bias = centred(splits[15], (ELEM, HID), 0.5, 3.0, (), jnp.float32)
    short_mid = centred(splits[16], (HID, ELEM, HID), HID ** -0.5, 1.0)
    short_out = centred(splits[17], (ELEM, HID), HID ** -0.5, 1.0, (), jnp.float32)
    short_offset = centred(splits[18], (ELEM,), 1.0, 3.0, (), jnp.float32)
    return {"positions": positions, "elements": elements, "prior_charges": prior_charges, "neighbours": neighbours, "counts": counts, "boundary": boundary, "wave_numbers": wave_numbers, "hardness": hardness, "chi_first": chi_first, "chi_bias": chi_bias, "chi_mid": chi_mid, "chi_out": chi_out, "chi_offset": chi_offset, "short_first": short_first, "short_charge": short_charge, "short_bias": short_bias, "short_mid": short_mid, "short_out": short_out, "short_offset": short_offset}


DOMAIN = 22.0
SOFTENING = 22.0
SCREENING = 0.005
CUTOFF = 66.0
DAMPING = 0.1
COUPLING = 64.0
FEATURE_SCALE = 0.5
PAIR_STRENGTH = 1.0

def neighbour_offsets():
    table = []
    for first in range(3):
        for second in range(3):
            for third in range(3):
                if first * 9 + second * 3 + third != 13:
                    table.append((first - 1, second - 1, third - 1))
    return table

def pair_terms(own_place, gathered, slot_counts):
    slots = gathered.shape[2]
    separation = gathered[:3] - own_place[:, :, None]
    distance = jnp.sqrt(lax.optimization_barrier(jnp.sum(separation * separation, axis=0)))
    valid = (jnp.arange(slots, dtype=jnp.int32)[None, :] < slot_counts[:, None]).astype(jnp.float32)
    soft = jnp.sqrt(distance * distance + SOFTENING * SOFTENING)
    kernel = valid * (PAIR_STRENGTH / slots) * SOFTENING * lax.erfc(SCREENING * soft) / soft
    spacing = CUTOFF / (NBASIS - 1)
    centres = spacing * jnp.arange(NBASIS, dtype=jnp.float32)
    taper = valid * 0.5 * (1.0 + jnp.cos(jnp.pi * jnp.minimum(distance, CUTOFF) / CUTOFF))
    basis = jnp.exp(-0.5 * ((distance[None] - centres[:, None, None]) / spacing) ** 2) * taper[None]
    return (kernel, basis)

def element_network(features, kinds, weight_first, bias, weight_mid, weight_out, offset, extra):
    count, hidden, width = weight_first.shape
    activation = jnp.dot(weight_first.reshape(count * hidden, width), features, preferred_element_type=jnp.float32)
    activation = activation + bias.reshape(count * hidden, 1) + extra
    mask = jnp.repeat(kinds, hidden, axis=0)
    first = (jnp.tanh(activation) * mask).astype(jnp.bfloat16)
    second = jnp.tanh(jnp.dot(weight_mid.reshape(hidden, count * hidden), first, preferred_element_type=jnp.float32))
    chosen = lax.optimization_barrier(jnp.sum(weight_out[:, :, None] * kinds[:, None, :], axis=0))
    return lax.optimization_barrier(jnp.sum(second * chosen, axis=0)) + lax.optimization_barrier(jnp.sum(offset[:, None] * kinds, axis=0))

def phase_tile(waves, placed):
    theta = waves[0][:, None] * placed[0][None, :] + waves[1][:, None] * placed[1][None, :] + waves[2][:, None] * placed[2][None, :]
    return jnp.concatenate([jnp.cos(theta), jnp.sin(theta)], axis=0)

def ghosts(rows, boundary, move):
    picked = jnp.take_along_axis(rows, jnp.broadcast_to(boundary[None], (rows.shape[0],) + boundary.shape), axis=4)
    blocks = []
    for shift in neighbour_offsets():
        part = jnp.roll(picked, (-shift[0], -shift[1], -shift[2]), axis=(1, 2, 3))
        if move:
            moved = DOMAIN * jnp.array(shift, dtype=jnp.float32).reshape(3, 1, 1, 1, 1)
            part = jnp.concatenate([part[:3] + moved, part[3:]], axis=0)
        blocks.append(part)
    return jnp.concatenate(blocks, axis=4)

def reference(positions, elements, prior_charges, neighbours, counts, boundary, wave_numbers, hardness, chi_first, chi_bias, chi_mid, chi_out, chi_offset, short_first, short_charge, short_bias, short_mid, short_out, short_offset):
    domains = NGX * NGY * NGZ
    atoms = ATOMS_DEV
    highest = lax.Precision.HIGHEST
    kinds = (elements[None] == jnp.arange(ELEM, dtype=jnp.int32).reshape(ELEM, 1, 1, 1, 1)).astype(jnp.float32)
    rows = jnp.concatenate([positions, kinds, prior_charges[None]], axis=0)
    width = rows.shape[0]
    extended = jnp.concatenate([rows, ghosts(rows, boundary, True)], axis=4).reshape(width, domains, -1).transpose(1, 0, 2)
    own_places = positions.reshape(3, domains, atoms).transpose(1, 0, 2)
    lists = neighbours.reshape(domains, atoms, NBR)
    slot_counts = counts.reshape(domains, atoms)

    def geometry(inputs):
        own_place, ext_rows, near, count = inputs
        gathered = ext_rows[:, near]
        kernel, basis = pair_terms(own_place, gathered, count)
        descriptor = jnp.einsum('mis,eis->emi', basis, gathered[3:3 + ELEM], precision=highest)
        return (kernel, descriptor.reshape(FEAT, atoms))
    kernel, descriptor = lax.map(geometry, (own_places, extended, lists, slot_counts))
    descriptor_all = descriptor.transpose(1, 0, 2).reshape(FEAT, domains * atoms)
    onehot = kinds.reshape(ELEM, domains * atoms)
    features = (FEATURE_SCALE * descriptor_all).astype(jnp.bfloat16)
    negativity = element_network(features, onehot, chi_first, chi_bias, chi_mid, chi_out, chi_offset, 0.0).reshape(domains, atoms)
    stiffness = lax.optimization_barrier(jnp.sum(hardness[:, None] * onehot, axis=0)).reshape(domains, atoms)
    grid = jnp.stack(jnp.meshgrid(jnp.arange(NGX), jnp.arange(NGY), jnp.arange(NGZ), indexing='ij')).astype(jnp.float32)
    placed = (positions + DOMAIN * grid[..., None]).reshape(3, domains, atoms).transpose(1, 0, 2)
    box = DOMAIN * jnp.array([NGX, NGY, NGZ], dtype=jnp.float32)
    waves = 2.0 * jnp.pi * wave_numbers.astype(jnp.float32) / box[:, None]
    squared = lax.optimization_barrier(jnp.sum(waves * waves, axis=0))
    wave_weights = COUPLING * DAMPING ** 2 * jnp.exp(-squared / (4.0 * DAMPING ** 2)) / (squared * (domains * atoms))
    wave_weights = jnp.concatenate([wave_weights, wave_weights])

    def structure(vector):

        def add_domain(total, item):
            return (total + jnp.dot(phase_tile(waves, item[0]), item[1], precision=highest), None)
        total, ignored = lax.scan(add_domain, jnp.zeros((2 * KVEC,), jnp.float32), (placed, vector))
        return total

    def spread(weighted):
        return lax.map(lambda place: jnp.dot(weighted, phase_tile(waves, place), precision=highest), placed)

    def apply(vector):
        ghost_values = ghosts(vector.reshape(1, NGX, NGY, NGZ, atoms), boundary, False).reshape(domains, -1)
        ext_values = jnp.concatenate([vector, ghost_values], axis=1)
        near_values = jax.vmap(lambda values, near: values[near])(ext_values, lists)
        return stiffness * vector + lax.optimization_barrier(jnp.sum(kernel * near_values, axis=2)) + spread(wave_weights * structure(vector))
    charges = prior_charges.reshape(domains, atoms)
    residual = -negativity - apply(charges)
    direction = residual
    norm_now = jnp.sum(residual * residual)
    for step in range(ITERS):
        image = apply(direction)
        alpha = norm_now / jnp.sum(direction * image)
        charges = charges + alpha * direction
        residual = residual - alpha * image
        norm_next = jnp.sum(residual * residual)
        direction = residual + norm_next / norm_now * direction
        norm_now = norm_next
    ghost_charge = ghosts(charges.reshape(1, NGX, NGY, NGZ, atoms), boundary, False).reshape(domains, -1)
    extended_charge = jnp.concatenate([charges, ghost_charge], axis=1)

    def charge_geometry(inputs):
        own_place, ext_rows, near, count, values = inputs
        gathered = ext_rows[:, near]
        ignored, basis = pair_terms(own_place, gathered, count)
        weighted_kinds = gathered[3:3 + ELEM] * values[near][None]
        return jnp.einsum('mis,eis->emi', basis, weighted_kinds, precision=highest).reshape(FEAT, atoms)
    charge_descriptor = lax.map(charge_geometry, (own_places, extended, lists, slot_counts, extended_charge))
    charge_all = charge_descriptor.transpose(1, 0, 2).reshape(FEAT, domains * atoms)
    inputs_short = (FEATURE_SCALE * jnp.concatenate([descriptor_all, charge_all], axis=0)).astype(jnp.bfloat16)
    flat_charges = charges.reshape(domains * atoms)
    energies = element_network(inputs_short, onehot, short_first, short_bias, short_mid, short_out, short_offset, short_charge.reshape(-1, 1) * flat_charges[None, :])
    return (charges.reshape(NGX, NGY, NGZ, atoms), energies.reshape(NGX, NGY, NGZ, atoms))
```

```python
import functools
import math

import jax
import jax.numpy as jnp
from jax import lax
from jax.experimental import pallas as pl
from jax.experimental.pallas import tpu as pltpu
from jax.sharding import PartitionSpec as P

ATOMS = 128
ELEM = 4
HID = 32
NBASIS = 32
ITERS = 3
AXES = ("gx", "gy", "gz")

DOMAIN = 22.0
SOFTENING = 22.0
SCREENING = 0.005
CUTOFF = 66.0
DAMPING = 0.1
COUPLING = 64.0
FEATURE_SCALE = 0.5
PAIR_STRENGTH = 1.0

STAGES = ("gy", "gx", "gz")
OFFSETS = [(a, b, c) for a in (-1, 0, 1) for b in (-1, 0, 1) for c in (-1, 0, 1) if (a, b, c) != (0, 0, 0)]
BLOCKS = len(OFFSETS)
WAVE_LANES = 96

F32 = jnp.float32
BF16 = jnp.bfloat16
HIGHEST = lax.Precision.HIGHEST


def iota(shape, dim):
    return lax.broadcasted_iota(jnp.int32, shape, dim)


def take_lanes(table, lanes):
    return jnp.take_along_axis(table, lanes, axis=1, mode="promise_in_bounds")


def dot(a, b, precision=None):
    return lax.dot_general(a, b, (((1,), (0,)), ((), ())), precision=precision, preferred_element_type=F32)


def total(x):
    return jnp.sum(jnp.sum(x, axis=0, keepdims=True), axis=1, keepdims=True)


def kernel(
    sizes,
    positions, elements, prior, neighbours, counts, boundary, waves,
    hardness, chi_first, chi_bias, chi_mid, chi_out, chi_offset,
    short_first, short_charge, short_bias, short_mid, short_out, short_offset,
    charges_out, energies_out,
    own_rows, places_in, places_got, row_out, row_got, part_out, gy_got, gx_got, gz_got,
    lanes, chunks, seen, pair, falloff, spans, tables, harmonics, phases, phases_t, coarse, ledger,
    halo_send, halo_recv, sum_send, sum_recv,
):
    at = {name: lax.axis_index(name) for name in AXES}

    def stepped(name, shift):
        return lax.rem(at[name] + (shift + sizes[name]), sizes[name])

    def device(shift):
        return tuple(stepped(name, s) if s else at[name] for name, s in zip(AXES, shift))

    partners = set(OFFSETS)
    for place, name in enumerate(AXES):
        for step in range(1, sizes[name]):
            step = step if step <= sizes[name] // 2 else step - sizes[name]
            partners.add(tuple(step if place == axis else 0 for axis in range(3)))
    barrier = pltpu.get_barrier_semaphore()
    for shift in sorted(partners):
        pl.semaphore_signal(barrier, inc=1, device_id=device(shift), device_id_type=pl.DeviceIdType.MESH)

    def send_blocks(source, slots, index):
        for number, shift in enumerate(OFFSETS):
            pltpu.make_async_remote_copy(
                src_ref=source, dst_ref=slots.at[number],
                send_sem=halo_send.at[index], recv_sem=halo_recv.at[index],
                device_id=device(tuple(-s for s in shift)), device_id_type=pl.DeviceIdType.MESH,
            ).start()

    def wait_blocks(slots, sems, index):
        pltpu.make_async_copy(slots, slots, sems.at[index]).wait()

    got = {"gy": gy_got, "gx": gx_got, "gz": gz_got}

    def send_part(number, stage, value):
        name = STAGES[stage]
        part_out[number, stage] = value
        for step in range(1, sizes[name]):
            pltpu.make_async_remote_copy(
                src_ref=part_out.at[number, stage], dst_ref=got[name].at[number, step - 1],
                send_sem=sum_send.at[number, stage], recv_sem=sum_recv.at[number, stage],
                device_id=device(tuple(step if axis == name else 0 for axis in AXES)),
                device_id_type=pl.DeviceIdType.MESH,
            ).start()

    def summed(number, stage, value):
        slots = got[STAGES[stage]].at[number]
        pltpu.make_async_copy(slots, slots, sum_recv.at[number, stage]).wait()
        for step in range(1, sizes[STAGES[stage]]):
            value = value + got[STAGES[stage]][number, step - 1]
        return value

    row8 = iota((8, ATOMS), 0)
    lane8 = iota((8, ATOMS), 1)

    own_rows[...] = jnp.zeros((8, ATOMS), F32)
    for axis in range(3):
        own_rows[axis:axis + 1, :] = positions[axis, 0, 0]
    element = elements[0, 0]
    own_rows[3:4, :] = element.astype(F32)
    own_rows[4:5, :] = prior[0, 0]
    own = own_rows[...]

    ledger[0] = jnp.zeros((8, ATOMS), F32)
    ledger[0, 0:1, 0:32] = boundary[0, 0].astype(F32)
    picks = ledger[0]
    picks = picks + pltpu.roll(picks, 32, 1)
    picks = picks + pltpu.roll(picks, 64, 1)
    picks = jnp.broadcast_to(picks[0:1, :], (8, ATOMS)).astype(jnp.int32)
    places_in[...] = take_lanes(own, picks)

    pl.semaphore_wait(barrier, len(partners))
    send_blocks(places_in, places_got, 0)

    lengths = [DOMAIN * sizes[name] for name in AXES]

    def harmonics_of(places):
        for axis, name in enumerate(AXES):
            angle = (2.0 * math.pi / lengths[axis]) * (places[axis] + DOMAIN * at[name].astype(F32))
            c1, s1 = jnp.cos(angle), jnp.sin(angle)
            c, s = c1, s1
            for order in range(8):
                harmonics[2 * axis, order] = c
                harmonics[2 * axis + 1, order] = s
                c, s = c * c1 - s * s1, s * c1 + c * s1

    def first_factors(row):
        return jnp.concatenate([harmonics[0, :, row, :], harmonics[1, :, row, :]], axis=0)

    def phases_of(row):
        zc, zs = harmonics[4, :, row, :], harmonics[5, :, row, :]
        sums_c, sums_s, gaps_c, gaps_s = [], [], [], []
        for order in range(6):
            yc = jnp.broadcast_to(harmonics[2, order, row:row + 1, :], (8, ATOMS))
            ys = jnp.broadcast_to(harmonics[3, order, row:row + 1, :], (8, ATOMS))
            cc, ss, sc, cs = yc * zc, ys * zs, ys * zc, yc * zs
            sums_c.append(cc - ss)
            sums_s.append(sc + cs)
            gaps_c.append(cc + ss)
            gaps_s.append(sc - cs)
        rest = [jnp.zeros((ATOMS - WAVE_LANES, ATOMS), F32)]
        return jnp.concatenate(sums_c + gaps_c + rest + sums_s + gaps_s + rest, axis=0)

    harmonics_of([jnp.broadcast_to(own[axis:axis + 1, :], (8, ATOMS)) for axis in range(3)])
    own_first = first_factors(0)
    own_phases = phases_of(0)
    phases[...] = own_phases
    phases_t[...] = own_phases.T

    def structure(vector):
        return dot(own_first * vector, phases_t[...], HIGHEST)

    def packed(s):
        return jnp.concatenate([s[:, 0:ATOMS], s[:, ATOMS:]], axis=0)

    part = packed(structure(own[4:5, :]))
    send_part(0, 0, part)

    kx, ky, kz = waves[0:1, :], waves[1:2, :], waves[2:3, :]
    flip = jnp.where(kx > 0, 1, -1)
    ky, kz = ky * flip, kz * flip
    order = jnp.abs(kx) - 1
    spot = jnp.where(ky * kz > 0, 0, 48) + (jnp.abs(ky) - 1) * 8 + jnp.abs(kz) - 1
    waves_n = waves.shape[1]
    left = jnp.where(ky > 0, order, order + 8)
    left = (iota((16, waves_n), 0) == left).astype(F32).astype(BF16)
    right = (iota((ATOMS, waves_n), 0) == spot).astype(F32).astype(BF16)
    tally = lax.dot_general(left, right, (((1,), (1,)), ((), ())), preferred_element_type=F32)
    sign_lane = jnp.where(lane8 >= 48, lane8 - 48, lane8)
    mid_order = lax.shift_right_logical(sign_lane, 3) + 1
    last_order = jnp.bitwise_and(sign_lane, 7) + 1
    squared = jnp.zeros((8, ATOMS), F32)
    for axis, number in enumerate((row8 + 1, mid_order, last_order)):
        wave = (2.0 * math.pi / lengths[axis]) * number.astype(F32)
        squared = squared + wave * wave
    all_atoms = ATOMS * sizes["gx"] * sizes["gy"] * sizes["gz"]
    weight = COUPLING * DAMPING**2 * jnp.exp(-squared / (4.0 * DAMPING**2)) / (squared * all_atoms)
    even = weight * (tally[0:8] + tally[8:16])
    odd = weight * (tally[0:8] - tally[8:16])

    def weighted(s):
        cc, sc, cs, ss = s[0:8], s[8:16], s[16:24], s[24:32]
        return jnp.concatenate(
            [even * cc - odd * ss, even * sc + odd * cs, even * cs + odd * sc, even * ss - odd * cc], axis=0
        )

    ledger[0] = jnp.zeros((8, ATOMS), F32)
    for number, table in enumerate((chi_bias, short_bias, short_charge, chi_out, short_out)):
        for kind in range(ELEM):
            ledger[0, number:number + 1, kind * HID:(kind + 1) * HID] = table[kind:kind + 1, :]
    columns = jnp.concatenate([ledger[0], jnp.zeros((ATOMS - 8, ATOMS), F32)], axis=0).T

    owns = [(element == kind).astype(F32) for kind in range(ELEM)]
    stiffness = functools.reduce(lambda a, b: a + b, [hardness[kind] * owns[kind] for kind in range(ELEM)])
    unit_kind = lax.shift_right_logical(iota((ATOMS, ATOMS), 0), 5)
    unit_mask = (unit_kind == element).astype(F32)

    def network(inputs, weights, bias, mid, out_column, offset, extra=None):
        activation = dot(weights, inputs) + columns[:, bias:bias + 1]
        if extra is not None:
            activation = activation + extra
        first = (jnp.tanh(activation) * unit_mask).astype(BF16)
        second = jnp.tanh(dot(mid, first))
        chosen = jnp.zeros((HID, ATOMS), F32)
        for kind in range(ELEM):
            chosen = chosen + columns[kind * HID:(kind + 1) * HID, out_column:out_column + 1] * owns[kind]
        result = jnp.sum(second * chosen, axis=0, keepdims=True)
        for kind in range(ELEM):
            result = result + offset[kind] * owns[kind]
        return result

    listed = neighbours[0, 0, 0].astype(F32).T.astype(jnp.int32)
    lanes[...] = jnp.bitwise_and(listed, ATOMS - 1)
    chunks[...] = lax.shift_right_logical(listed, 7)

    block = 4 * (row8 - 1) + lax.shift_right_logical(lane8, 5)

    def extended(own_row, slots, row):
        value = jnp.where(row8 == 0, own_row, 0.0)
        for number in range(BLOCKS):
            value = jnp.where(block == number, slots[number, row:row + 1, :], value)
        return value

    def gathered(values):
        result = None
        which = chunks[...]
        where = lanes[...]
        for number in range(8):
            table = jnp.broadcast_to(values[number:number + 1, :], (ATOMS, ATOMS))
            picked = take_lanes(table, where)
            result = picked if result is None else jnp.where(which == number, picked, result)
        return result

    wait_blocks(places_got, halo_recv, 0)
    offset_index = jnp.where(block >= 13, block + 1, block)
    digit_x = jnp.where(offset_index >= 18, 1, jnp.where(offset_index >= 9, 0, -1))
    within = offset_index - 9 * (digit_x + 1)
    digit_y = jnp.where(within >= 6, 1, jnp.where(within >= 3, 0, -1))
    digit_z = within - 3 * (digit_y + 1) - 1
    ghost = (row8 > 0) & (block < BLOCKS)
    spaces = []
    for axis, digit in enumerate((digit_x, digit_y, digit_z)):
        spaces.append(extended(own[axis:axis + 1, :], places_got, axis) + jnp.where(ghost, DOMAIN * digit.astype(F32), 0.0))
    kinds = extended(own[3:4, :], places_got, 3)
    charge = extended(own[4:5, :], places_got, 4)

    apart = jnp.zeros((ATOMS, ATOMS), F32)
    for axis in range(3):
        gap = gathered(spaces[axis]) - own[axis:axis + 1, :]
        apart = apart + gap * gap
    distance = jnp.sqrt(apart)
    valid = (iota((ATOMS, ATOMS), 0) < counts[0, 0]).astype(F32)
    soft = jnp.sqrt(apart + SOFTENING * SOFTENING)
    pair[...] = valid * (PAIR_STRENGTH / ATOMS) * SOFTENING * (1.0 - lax.erf(SCREENING * soft)) / soft
    falloff[...] = valid * 0.5 * (1.0 + jnp.cos(math.pi * jnp.minimum(distance, CUTOFF) / CUTOFF))
    spans[...] = distance
    near_kinds = gathered(kinds)
    for kind in range(ELEM):
        seen[kind] = (near_kinds == float(kind)).astype(F32)

    part = summed(0, 0, part)
    send_part(0, 1, part)

    def local_part(values):
        return stiffness * values[0:1, :] + jnp.sum(pair[...] * gathered(values), axis=0, keepdims=True)

    spacing = CUTOFF / (NBASIS - 1)

    def descriptors(base):
        def step(number, carry):
            centre = spacing * lax.convert_element_type(number, F32)
            scaled = (spans[...] - centre) / spacing
            basis = jnp.exp(-0.5 * (scaled * scaled)) * falloff[...]
            for kind in range(ELEM):
                tables[pl.ds(base + kind * NBASIS + number, 1), :] = jnp.sum(basis * seen[kind], axis=0, keepdims=True)
            return carry
        lax.fori_loop(0, NBASIS, step, 0)

    start_local = local_part(charge)
    descriptors(0)
    part = summed(0, 1, part)
    send_part(0, 2, part)
    features = (FEATURE_SCALE * tables[0:ATOMS, :]).astype(BF16)
    negativity = network(features, chi_first[...], 0, chi_mid[...], 3, chi_offset)

    def send_row(row, index):
        row_out[index] = take_lanes(jnp.broadcast_to(row, (8, ATOMS)), picks)[0:1, :]
        send_blocks(row_out.at[index], row_got.at[index], index + 1)

    def extended_row(row, index):
        wait_blocks(row_got.at[index], halo_recv, index + 1)
        return extended(row, row_got.at[index], 0)

    known = negativity + start_local
    send_row(known, 0)

    harmonics_of(spaces)
    ghost_first = []
    for row in range(1, 8):
        ghost_first.append(first_factors(row))
        coarse[:, (row - 1) * ATOMS:row * ATOMS] = phases_of(row).astype(BF16)

    def spread(u):
        u = jnp.concatenate([u[0:16], u[16:32]], axis=1)
        mine = jnp.sum(own_first * dot(u, phases[...], HIGHEST), axis=0, keepdims=True)
        value = jnp.where(row8 == 0, mine, 0.0)
        theirs = dot(u.astype(BF16), coarse[...])
        for row in range(1, 8):
            piece = jnp.sum(ghost_first[row - 1] * theirs[:, (row - 1) * ATOMS:row * ATOMS], axis=0, keepdims=True)
            value = jnp.where(row8 == row, piece, value)
        return jnp.where((row8 == 0) | ghost, value, 0.0)

    part = summed(0, 2, part)
    potential = spread(weighted(part))
    residual = -(extended_row(known, 0) + potential)

    direction = image = local_direction = shape_direction = curvature = norm = None
    for step in range(ITERS):
        mine = residual[0:1, :]
        local = local_part(residual)
        rows = [mine * mine, mine * local]
        if step:
            rows += [mine * local_direction, direction[0:1, :] * local]
        products = jnp.concatenate(rows + [jnp.zeros((8 - len(rows), ATOMS), F32)], axis=0)
        products = jnp.sum(products, axis=1, keepdims=True)
        part = packed(structure(mine))
        top = jnp.where(lane8 == WAVE_LANES, products, part[0:8])
        part = jnp.concatenate([top, part[8:32]], axis=0)
        send_part(step + 1, 0, part)
        if step + 1 < ITERS:
            send_row(local, step + 1)
        part = summed(step + 1, 0, part)
        send_part(step + 1, 1, part)
        part = summed(step + 1, 1, part)
        send_part(step + 1, 2, part)
        part = summed(step + 1, 2, part)
        sums = [part[number:number + 1, WAVE_LANES:WAVE_LANES + 1] for number in range(4)]
        u = weighted(part)
        energy = part * u
        energy = total(energy[0:8] + energy[8:16] + energy[16:24] + energy[24:32])
        own_curvature = sums[1] + energy
        if step == 0:
            curvature = own_curvature
            direction, local_direction, shape_direction = residual, local, part
        else:
            ratio = sums[0] / norm
            cross = shape_direction * u
            cross = 2.0 * total(cross[0:8] + cross[8:16] + cross[16:24] + cross[24:32]) + sums[2] + sums[3]
            curvature = own_curvature + ratio * cross + ratio * ratio * curvature
            direction = residual + ratio * direction
            local_direction = local + ratio * local_direction
            shape_direction = part + ratio * shape_direction
        norm = sums[0]
        alpha = norm / curvature
        charge = charge + alpha * direction
        if step + 1 < ITERS:
            fresh = extended_row(local, step + 1) + spread(u)
            image = fresh if step == 0 else fresh + ratio * image
            residual = residual - alpha * image

    charges_out[0, 0] = charge[0:1, :]
    near_charge = gathered(charge)
    for kind in range(ELEM):
        seen[kind] = seen[kind] * near_charge
    descriptors(ATOMS)
    inputs = (FEATURE_SCALE * tables[...]).astype(BF16)
    energies_out[0, 0] = network(
        inputs, short_first[...], 1, short_mid[...], 4, short_offset,
        columns[:, 2:3] * charge[0:1, :],
    )

    wait_blocks(places_got, halo_send, 0)
    for index in range(ITERS):
        wait_blocks(row_got.at[index], halo_send, index + 1)
    for number in range(ITERS + 1):
        for stage, name in enumerate(STAGES):
            slots = got[name].at[number]
            pltpu.make_async_copy(slots, slots, sum_send.at[number, stage]).wait()


def solution(mesh):
    sizes = {name: mesh.shape[name] for name in AXES}

    def body(
        positions, elements, prior_charges, neighbours, counts, boundary, wave_numbers, hardness,
        chi_first, chi_bias, chi_mid, chi_out, chi_offset,
        short_first, short_charge, short_bias, short_mid, short_out, short_offset,
    ):
        vmem, smem = pl.BlockSpec(memory_space=pltpu.VMEM), pl.BlockSpec(memory_space=pltpu.SMEM)
        sums = ITERS + 1
        return pl.pallas_call(
            functools.partial(kernel, sizes),
            out_shape=[jax.ShapeDtypeStruct((1, 1, 1, ATOMS), F32)] * 2,
            in_specs=[vmem] * 7 + [smem] + [vmem] * 4 + [smem] + [vmem] * 5 + [smem],
            out_specs=[vmem] * 2,
            scratch_shapes=[
                pltpu.VMEM((8, ATOMS), F32),
                pltpu.VMEM((8, ATOMS), F32),
                pltpu.VMEM((BLOCKS, 8, ATOMS), F32),
                pltpu.VMEM((ITERS, 1, ATOMS), F32),
                pltpu.VMEM((ITERS, BLOCKS, 1, ATOMS), F32),
                pltpu.VMEM((sums, 3, 32, ATOMS), F32),
                pltpu.VMEM((sums, sizes["gy"] - 1, 32, ATOMS), F32),
                pltpu.VMEM((sums, sizes["gx"] - 1, 32, ATOMS), F32),
                pltpu.VMEM((sums, sizes["gz"] - 1, 32, ATOMS), F32),
                pltpu.VMEM((ATOMS, ATOMS), jnp.int32),
                pltpu.VMEM((ATOMS, ATOMS), jnp.int32),
                pltpu.VMEM((ELEM, ATOMS, ATOMS), F32),
                pltpu.VMEM((ATOMS, ATOMS), F32),
                pltpu.VMEM((ATOMS, ATOMS), F32),
                pltpu.VMEM((ATOMS, ATOMS), F32),
                pltpu.VMEM((2 * ATOMS, ATOMS), F32),
                pltpu.VMEM((6, 8, 8, ATOMS), F32),
                pltpu.VMEM((2 * ATOMS, ATOMS), F32),
                pltpu.VMEM((ATOMS, 2 * ATOMS), F32),
                pltpu.VMEM((2 * ATOMS, 7 * ATOMS), BF16),
                pltpu.VMEM((1, 8, ATOMS), F32),
                pltpu.SemaphoreType.DMA((ITERS + 1,)),
                pltpu.SemaphoreType.DMA((ITERS + 1,)),
                pltpu.SemaphoreType.DMA((sums, 3)),
                pltpu.SemaphoreType.DMA((sums, 3)),
            ],
            compiler_params=pltpu.CompilerParams(collective_id=0, has_side_effects=True),
        )(
            positions, elements, prior_charges, neighbours, counts, boundary.reshape(1, 1, 1, -1), wave_numbers,
            hardness, chi_first.reshape(ELEM * HID, -1), chi_bias, chi_mid.reshape(HID, -1), chi_out, chi_offset,
            short_first.reshape(ELEM * HID, -1), short_charge, short_bias, short_mid.reshape(HID, -1), short_out,
            short_offset,
        )

    cell = P("gx", "gy", "gz", None)
    return jax.shard_map(
        body,
        mesh=mesh,
        in_specs=(P(None, *cell), cell, cell, P(*cell, None), cell, cell) + (P(),) * 13,
        out_specs=(cell, cell),
        check_vma=False,
    )
```
